32 devices in a mesh: groups: 2 (over y), batch: 4 (over z), blk: 4 (over x, core).
Axes of the slice: x: 2, y: 2, z: 4, core: 2. Of those that a mesh axis runs over, the one named last changes fastest.
Arguments:
- queries: bfloat16 [8, 592, 1024], P(('groups', 'batch'), 'blk'), parts along dimension 0, may hold values from -12 to 12
- key_states: bfloat16 [8, 592, 1024], P(('groups', 'batch'), 'blk'), parts along dimension 0, may hold values from -6 to 6
- value_states: bfloat16 [8, 592, 1024], P(('groups', 'batch'), 'blk'), parts along dimension 0, may hold values from -6 to 6
- residual: bfloat16 [8, 592, 768], P(('groups', 'batch'), 'blk'), parts along dimension 0, may hold values from -3 to 3
- proj_weight: bfloat16 [1024, 768], P(None, 'batch'), may hold values from -0.1875 to 0.1875
- conv_weight: bfloat16 [3, 3, 768, 384], P(None, None, 'batch'), may hold values from -0.078125 to 0.078125
Outputs:
- conv_out: bfloat16 [8, 592, 384], P(('groups', 'batch'), 'blk'), parts along dimension 0
The draws below stay inside these ranges and needn't reach their ends.
There are 2 independent parts, one for each index of `groups`. The reference program is written for one: setup_inputs(seed, part) draws one part's arguments, and reference() takes and returns one part's arrays. A program takes and returns all parts, laid end to end along the dimension named above; an argument that names none is the same for every part. Nothing has to cross between parts.
All inputs are finite; a program needn't handle non-finite values.
Results may differ from the reference program's by a relative error of at most 0.0085.
Values may be sent and summed in bfloat16 or wider, within the bound.
No kernel may reach another device: no remote copies, remote signals or barrier semaphores. Data moves between devices by JAX's collectives and lax.ppermute only.
A program may use at most 64 MiB of HBM per device.

```python
import jax
import jax.numpy as jnp
from jax import lax

HEADS = 16
HD = 64
FEATW = 768
FEAT = 384
COLS = 74
NROWS = 8
TOKENS = 592
IMAGES = 4


def draw_queries(key, part):
    base_draw = 3.0 * jnp.clip(jax.random.normal(jax.random.fold_in(key, 1), (IMAGES, TOKENS, HEADS * HD), jnp.float32), -4.0, 4.0)
    return base_draw.astype(jnp.bfloat16)


def draw_key_states(key, part):
    base_draw = jnp.clip(jax.random.normal(jax.random.fold_in(key, 2), (IMAGES, TOKENS, HEADS * HD), jnp.float32), -6.0, 6.0)
    return base_draw.astype(jnp.bfloat16)


def levels(key, shape, shards, low, largest):
    level, own = 1.0, jax.random.fold_in(key, 6)
    for position, blocks in shards:
        steps = jnp.exp(jax.random.uniform(jax.random.fold_in(own, position), (blocks,), jnp.float32, low / len(shards), largest / len(shards)))
        level = level * jnp.repeat(steps, shape[position] // blocks).reshape([-1 if axis == position else 1 for axis in range(len(shape))])
    return level


def gaussian(rng, dims, deviation, bound, pieces=(), kind=jnp.bfloat16):
    result = jax.random.normal(rng, dims, jnp.float32) * deviation
    if len(pieces) > 0:
        result = levels(rng, dims, pieces, -0.22, 0.18) * result
    return jnp.clip(result, min=-bound, max=bound).astype(kind)


def setup_inputs(seed: int = 0, part: int = 0) -> dict:
    key_of = jax.random.split(jax.random.key(seed), 7)
    part_keys = jax.random.split(jax.random.fold_in(key_of[6], part), 7)
    queries = draw_queries(jax.random.fold_in(jax.random.fold_in(key_of[6], part), 71), part)
    key_states = draw_key_states(jax.random.fold_in(jax.random.fold_in(key_of[6], part), 71), part)
    value_states = gaussian(part_keys[2], (IMAGES, TOKENS, HEADS * HD), 1.0, 6.0, ((0, 4), (1, 4)))
    residual = gaussian(part_keys[3], (IMAGES, TOKENS, FEATW), 0.5, 3.0, ((0, 4), (1, 4)))
    proj_weight = gaussian(key_of[4], (HEADS * HD, FEATW), (HEADS * HD) ** -0.5, 0.1875, ((1, 4),))
    conv_weight = gaussian(key_of[5], (3, 3, FEATW, FEAT), (9 * FEATW) ** -0.5, 0.078125, ((2, 4),))
    return dict(queries=queries, key_states=key_states, value_states=value_states, residual=residual, proj_weight=proj_weight, conv_weight=conv_weight)


def one_head(head_args):
    query_head, key_head, value_head = head_args
    scores = jnp.dot(query_head, key_head.T, preferred_element_type=jnp.float32) * (HD ** -0.5)
    row_max = jnp.max(scores, axis=1, keepdims=True)
    weights = jnp.exp(scores - row_max)
    weight_sum = jnp.sum(weights, axis=1, keepdims=True)
    mixed = jnp.dot(weights.astype(jnp.bfloat16), value_head, preferred_element_type=jnp.float32)
    return mixed / weight_sum


def one_image(image_args, proj_weight, conv_weight):
    queries, key_states, value_states, residual = image_args
    query_heads = queries.reshape(TOKENS, HEADS, HD).transpose(1, 0, 2)
    key_heads = key_states.reshape(TOKENS, HEADS, HD).transpose(1, 0, 2)
    value_heads = value_states.reshape(TOKENS, HEADS, HD).transpose(1, 0, 2)
    mixed = lax.map(one_head, (query_heads, key_heads, value_heads))
    attention = mixed.transpose(1, 0, 2).reshape(TOKENS, HEADS * HD).astype(jnp.bfloat16)
    projected = jnp.dot(attention, proj_weight, preferred_element_type=jnp.float32)
    hidden = (residual.astype(jnp.float32) + projected).astype(jnp.bfloat16)
    feature_grid = hidden.reshape(NROWS, COLS, FEATW)
    padded = jnp.pad(feature_grid, ((1, 1), (1, 1), (0, 0)))
    conv_sum = jnp.zeros((TOKENS, FEAT), jnp.float32)
    for row_off in range(3):
        for col_off in range(3):
            window = padded[row_off:row_off + NROWS, col_off:col_off + COLS].reshape(TOKENS, FEATW)
            conv_sum = conv_sum + jnp.dot(window, conv_weight[row_off, col_off], preferred_element_type=jnp.float32)
    return conv_sum.astype(jnp.bfloat16)


def reference(queries, key_states, value_states, residual, proj_weight, conv_weight):
    return lax.map(lambda image_args: one_image(image_args, proj_weight, conv_weight),
                   (queries, key_states, value_states, residual))
```

```python
import functools

import jax
import jax.numpy as jnp
from jax import lax
from jax.experimental import pallas as pl
from jax.experimental.pallas import tpu as pltpu
from jax.sharding import PartitionSpec as P

HD = 64
COLS = 74
PAIR = 2
FAR = 1


def attend(q_refs, kv_pairs, state, out_state, out_final):
    width = q_refs[0].shape[1]
    low = lax.broadcasted_iota(jnp.int32, (1, 2 * HD), 1) < HD
    for pair in range(width // (2 * HD)):
        lanes = slice(pair * 2 * HD, (pair + 1) * 2 * HD)
        for which, q_ref in enumerate(q_refs):
            q_tile = q_ref[:, lanes] * jnp.bfloat16(HD ** -0.5)
            halves = []
            for side in range(2):
                q_side = jnp.where(low if side == 0 else ~low, q_tile, jnp.zeros_like(q_tile))
                scores = [
                    lax.dot_general(q_side, k_ref[:, lanes], (((1,), (1,)), ((), ())), preferred_element_type=jnp.float32)
                    for k_ref, _ in kv_pairs
                ]
                row_max = functools.reduce(jnp.maximum, [jnp.max(s, axis=1, keepdims=True) for s in scores])
                if state is not None:
                    at = pair * 2 * HD + side * HD
                    old_max = state[0][which, :, at : at + 1]
                    row_max = jnp.maximum(row_max, old_max)
                total = 0.0
                mixed = 0.0
                for s, (_, v_ref) in zip(scores, kv_pairs):
                    weights = jnp.exp(s - row_max)
                    total = total + jnp.sum(weights, axis=1, keepdims=True)
                    mixed = mixed + jnp.dot(weights.astype(jnp.bfloat16), v_ref[:, lanes], preferred_element_type=jnp.float32)
                if state is not None:
                    factor = jnp.exp(old_max - row_max)
                    total = total + state[1][which, :, at : at + 1] * factor
                    mixed = mixed + state[2][which, :, lanes] * factor
                halves.append((row_max, total, mixed))
            (max_a, sum_a, mix_a), (max_b, sum_b, mix_b) = halves
            mix = jnp.where(low, mix_a, mix_b)
            tot = jnp.where(low, sum_a, sum_b)
            if out_final is not None:
                out_final(which, lanes, mix / tot)
            else:
                out_state[0][which, :, lanes] = jnp.where(low, max_a, max_b)
                out_state[1][which, :, lanes] = tot
                out_state[2][which, :, lanes] = mix


def attention_first(q_own, sib, kv_own, kv_far):
    rows, width = q_own.shape

    def kernel(q_ref, sib_ref, own_ref, far_ref, m_ref, l_ref, a_ref):
        w = width
        attend(
            [q_ref, sib_ref.at[:, 0:w]],
            [
                (own_ref.at[:, 0:w], own_ref.at[:, w : 2 * w]),
                (sib_ref.at[:, w : 2 * w], sib_ref.at[:, 2 * w : 3 * w]),
                (far_ref.at[:, 0:w], far_ref.at[:, w : 2 * w]),
            ],
            None,
            (m_ref, l_ref, a_ref),
            None,
        )

    shape = jax.ShapeDtypeStruct((2, rows, width), jnp.float32)
    return pl.pallas_call(kernel, out_shape=(shape, shape, shape), name="attention_first")(q_own, sib, kv_own, kv_far)


def attention_next(q_own, sib, kv_far, state):
    rows, width = q_own.shape

    def kernel(q_ref, sib_ref, far_ref, m_in, l_in, a_in, m_ref, l_ref, a_ref):
        w = width
        attend(
            [q_ref, sib_ref.at[:, 0:w]],
            [(far_ref.at[:, 0:w], far_ref.at[:, w : 2 * w])],
            (m_in, l_in, a_in),
            (m_ref, l_ref, a_ref),
            None,
        )

    shape = jax.ShapeDtypeStruct((2, rows, width), jnp.float32)
    return pl.pallas_call(kernel, out_shape=(shape, shape, shape), name="attention_next")(q_own, sib, kv_far, *state)


def attention_last(q_own, sib, kv_far, state, proj):
    rows, width = q_own.shape
    cols = proj[0].shape[1]
    parts = len(proj)

    def kernel(q_ref, sib_ref, far_ref, m_in, l_in, a_in, *refs):
        proj_refs, out_refs, mixed_ref = refs[:parts], refs[parts:-1], refs[-1]
        w = width

        def keep(which, lanes, value):
            mixed_ref[which, :, lanes] = value.astype(jnp.bfloat16)

        attend(
            [q_ref, sib_ref.at[:, 0:w]],
            [(far_ref.at[:, 0:w], far_ref.at[:, w : 2 * w])],
            (m_in, l_in, a_in),
            None,
            keep,
        )
        for part in range(parts):
            for which in range(2):
                out_refs[part // 2][which, :, part % 2 * cols : (part % 2 + 1) * cols] = jnp.dot(
                    mixed_ref[which], proj_refs[part][...], preferred_element_type=jnp.float32
                ).astype(out_refs[part // 2].dtype)

    return pl.pallas_call(
        kernel,
        out_shape=(
            jax.ShapeDtypeStruct((2, rows, 2 * cols), jnp.float32),
            jax.ShapeDtypeStruct((2, rows, 2 * cols), jnp.float32),
        ),
        scratch_shapes=[pltpu.VMEM((2, rows, width), jnp.bfloat16)],
        name="attention_last",
    )(q_own, sib, kv_far, *state, *proj)


def body(queries, key_states, value_states, residual, proj_weight, conv_weight):
    q_rows, k_rows, v_rows, res_rows = queries[0], key_states[0], value_states[0], residual[0]
    tokens, width = q_rows.shape
    feat_in = res_rows.shape[1]
    feat_out = conv_weight.shape[3]
    blk_count = lax.axis_size("blk")
    batch_count = lax.axis_size("batch")
    chips = blk_count // 2
    core = lax.axis_index("blk") % 2
    depth = lax.axis_index("batch")
    half = width // 2
    quarter = feat_in // 4

    def to_sibling(x):
        return lax.ppermute(x, "blk", [(i, i ^ 1) for i in range(blk_count)])

    def head_cols(x, which):
        return lax.dynamic_slice_in_dim(x, which * half, half, axis=1)

    kv_own = jnp.concatenate([head_cols(k_rows, core), head_cols(v_rows, core)], axis=1)
    kv_other = jnp.concatenate([head_cols(k_rows, 1 - core), head_cols(v_rows, 1 - core)], axis=1)
    q_own = head_cols(q_rows, core)
    sib_send = jnp.concatenate([head_cols(q_rows, 1 - core), kv_other], axis=1)
    far = []
    for step in range(1, chips):
        for cross, block in ((0, kv_own), (1, kv_other)):
            far.append(lax.ppermute(block, "blk", [(i, ((i ^ cross) + 2 * step) % blk_count) for i in range(blk_count)]))
    sib = to_sibling(sib_send)

    my_proj = lax.dynamic_slice_in_dim(proj_weight, core * half, half, axis=0)
    joint = ("batch", "blk")
    if batch_count == 4:

        def by_role(x, role, only_second):
            pairs = []
            for z in range(batch_count):
                for b in range(blk_count):
                    source = z ^ role ^ (FAR if b % 2 else 0)
                    pairs.append((source * blk_count + b, z * blk_count + b))
            return lax.ppermute(x, joint, pairs)

        proj = [by_role(my_proj, role, False) for role in (0, PAIR, FAR, PAIR ^ FAR)]
        taps = by_role(conv_weight, 0, True)
    else:
        all_proj = lax.all_gather(my_proj, "batch", axis=1, tiled=True)
        all_taps = lax.all_gather(conv_weight, "batch", axis=2, tiled=True)
        mine = (depth % 4) ^ (core * FAR)
        proj = [
            lax.dynamic_slice_in_dim(all_proj, (mine ^ role) * quarter, quarter, axis=1)
            for role in (0, PAIR, FAR, PAIR ^ FAR)
        ]
        taps = lax.dynamic_slice_in_dim(all_taps, mine * quarter, quarter, axis=2)

    def quarter_cols(x, index):
        return lax.dynamic_slice_in_dim(x, index * quarter, quarter, axis=1)

    mine = (depth % 4) ^ (core * FAR)
    res_mine = jnp.concatenate([quarter_cols(res_rows, mine), quarter_cols(res_rows, mine ^ PAIR)], axis=1)
    res_send = jnp.concatenate([quarter_cols(res_rows, mine ^ FAR), quarter_cols(res_rows, mine ^ FAR ^ PAIR)], axis=1)
    res_sib = to_sibling(res_send)

    state = attention_first(q_own, sib, kv_own, far[0])
    for block in far[1:-1]:
        state = attention_next(q_own, sib, block, state)
    part_mine, part_sib = attention_last(q_own, sib, far[-1], state, proj)

    part_recv = to_sibling(part_sib)
    own_sum = part_mine[0] + part_recv[1] + res_mine.astype(jnp.float32)
    sib_sum = part_mine[1] + part_recv[0] + res_sib.astype(jnp.float32)
    first = jnp.where(core == 0, own_sum, sib_sum).astype(jnp.bfloat16)
    second = jnp.where(core == 0, sib_sum, own_sum).astype(jnp.bfloat16)
    hidden = jnp.stack([first, second], axis=0)

    def to_pair(x):
        return lax.ppermute(x, "batch", [(i, i ^ PAIR) for i in range(batch_count)])

    kept, sent = hidden[:, :, :quarter], hidden[:, :, quarter:]
    got = to_pair(sent)
    grid = jnp.stack([kept, got], axis=0).reshape(2, 2 * tokens // COLS, COLS, quarter)
    above = lax.ppermute(grid[:, -1:], "blk", [(i, i + 2) for i in range(blk_count - 2)])
    below = lax.ppermute(grid[:, :1], "blk", [(i + 2, i) for i in range(blk_count - 2)])
    rimmed = jnp.concatenate([above, grid, below], axis=1)
    partial = lax.conv_general_dilated(
        rimmed,
        taps,
        (1, 1),
        ((0, 0), (1, 1)),
        dimension_numbers=("NHWC", "HWIO", "NHWC"),
        preferred_element_type=jnp.float32,
    ).reshape(2, 2, tokens, feat_out)
    mine_part = lax.dynamic_index_in_dim(partial, core, axis=1, keepdims=False)
    other_part = lax.dynamic_index_in_dim(partial, 1 - core, axis=1, keepdims=False)
    summed = mine_part + to_sibling(other_part)
    swapped = to_pair(summed[1].astype(jnp.bfloat16))
    return (summed[0] + swapped.astype(jnp.float32)).astype(jnp.bfloat16)[None]


def solution(mesh):
    return jax.shard_map(
        body,
        mesh=mesh,
        in_specs=(
            P(("groups", "batch"), "blk", None),
            P(("groups", "batch"), "blk", None),
            P(("groups", "batch"), "blk", None),
            P(("groups", "batch"), "blk", None),
            P(None, "batch"),
            P(None, None, "batch", None),
        ),
        out_specs=P(("groups", "batch"), "blk", None),
        check_vma=False,
    )
```

```python
import functools

import jax
import jax.numpy as jnp
from jax import lax
from jax.experimental import pallas as pl
from jax.experimental.pallas import tpu as pltpu
from jax.sharding import PartitionSpec as P

HD = 64
COLS = 74
STRIDE = 80
TAPS = 3
CHUNKS = ((0, 5), (5, 9))


def pack(scalars, q_rows, k_rows, v_rows, res_rows, count):
    tokens, width = q_rows.shape
    cols = width // count
    quarter = res_rows.shape[1] // count
    total = 3 * cols + quarter

    def kernel(s_ref, q_ref, k_ref, v_ref, r_ref, *outs):
        for d, out in enumerate(outs):
            at = pl.multiple_of((s_ref[0] ^ d) * cols, cols)
            for i, ref in enumerate((q_ref, k_ref, v_ref)):
                out[:, i * cols : (i + 1) * cols] = ref[:, pl.ds(at, cols)]
            for s in range(count):

                @pl.when(s_ref[2 + d] == s)
                def _():
                    out[:, 3 * cols :] = r_ref[:, s * quarter : (s + 1) * quarter]

    if cols % 128 == 0:
        return pl.pallas_call(
            kernel,
            out_shape=[jax.ShapeDtypeStruct((tokens, total), q_rows.dtype)] * count,
            in_specs=[pl.BlockSpec(memory_space=pltpu.SMEM)] + [pl.BlockSpec(memory_space=pltpu.VMEM)] * 4,
            name="pack",
        )(scalars, q_rows, k_rows, v_rows, res_rows)
    outs = []
    for d in range(count):
        at = (scalars[0] ^ d) * cols
        parts = [lax.dynamic_slice_in_dim(x, at, cols, axis=1) for x in (q_rows, k_rows, v_rows)]
        parts.append(lax.dynamic_slice_in_dim(res_rows, scalars[2 + d] * quarter, quarter, axis=1))
        outs.append(jnp.concatenate(parts, axis=1))
    return outs


def attention(scalars, blocks, cols):
    count = len(blocks)
    tokens = blocks[0].shape[0]
    lane = min(cols, 2 * HD)

    def kernel(s_ref, *refs):
        b_refs, out_ref, wide_ref, kv_ref = refs[:count], refs[count], refs[count + 1], refs[count + 2]
        for j, b_ref in enumerate(b_refs):
            wide_ref[j * tokens : (j + 1) * tokens, :] = b_ref[:, cols : 3 * cols].astype(jnp.float32)
        kv_ref[...] = wide_ref[...].astype(jnp.bfloat16)
        low = lax.broadcasted_iota(jnp.int32, (1, lane), 1) < HD
        for group in range(cols // lane):
            lanes = slice(group * lane, (group + 1) * lane)
            keys = kv_ref[:, lanes]
            values = kv_ref[:, cols + group * lane : cols + (group + 1) * lane]
            for j, b_ref in enumerate(b_refs):
                q_tile = b_ref[:, lanes] * jnp.bfloat16(HD ** -0.5)
                halves = []
                for side in range(lane // HD):
                    q_side = q_tile
                    if lane > HD:
                        q_side = jnp.where(low if side == 0 else ~low, q_tile, jnp.zeros_like(q_tile))
                    scores = lax.dot_general(q_side, keys, (((1,), (1,)), ((), ())), preferred_element_type=jnp.float32)
                    weights = jnp.exp(scores - jnp.max(scores, axis=1, keepdims=True))
                    total = jnp.sum(weights, axis=1, keepdims=True)
                    mixed = jnp.dot(weights.astype(jnp.bfloat16), values, preferred_element_type=jnp.float32)
                    halves.append(mixed / total)
                mix = halves[0] if len(halves) == 1 else jnp.where(low, halves[0], halves[1])
                out_ref[s_ref[0] ^ j, :, lanes] = mix.astype(jnp.bfloat16)

    return pl.pallas_call(
        kernel,
        out_shape=jax.ShapeDtypeStruct((count, tokens, cols), jnp.bfloat16),
        in_specs=[pl.BlockSpec(memory_space=pltpu.SMEM)] + [pl.BlockSpec(memory_space=pltpu.VMEM)] * count,
        scratch_shapes=[
            pltpu.VMEM((count * tokens, 2 * cols), jnp.float32),
            pltpu.VMEM((count * tokens, 2 * cols), jnp.bfloat16),
        ],
        name="attention",
    )(scalars, *blocks)


def project_and_convolve(scalars, mixed, blocks, proj_parts, tap_parts, feat_out):
    count = len(mixed)
    tokens, cols = mixed[0].shape[1:]
    quarter = blocks[0].shape[1] - 3 * cols
    rows = tokens // COLS
    grid_rows = rows * count
    margin = 8
    parts = len(proj_parts)

    def kernel(s_ref, *refs):
        m_refs, refs = refs[:count], refs[count:]
        b_refs, refs = refs[:count], refs[count:]
        p_refs, refs = refs[:parts], refs[parts:]
        t_refs, refs = refs[: len(tap_parts)], refs[len(tap_parts) :]
        even_ref, odd_ref, p_all, t_all, hid_ref, wide_ref, near_ref = refs
        me, side = s_ref[0], s_ref[1]
        if parts == 1:
            p_all[...] = p_refs[0][...].reshape(p_all.shape)
            for (t0, t1), t_ref in zip(CHUNKS, t_refs):
                t_all[t0:t1] = t_ref[...]
        else:
            share = count // 2
            for which, p_ref in enumerate(p_refs):
                p_all[pl.ds((side ^ which) * share, share)] = p_ref[...].reshape(share, cols, quarter)
            for i, t_ref in enumerate(t_refs):
                t0, t1 = CHUNKS[i // 2]
                at = pl.multiple_of((side ^ (i % 2)) * (quarter // 2), 16)
                t_all[t0:t1, pl.ds(at, quarter // 2), :] = t_ref[...]
        wide_ref[...] = jnp.zeros_like(wide_ref)
        for j in range(count):
            total = 0.0
            for d in range(count):
                total = total + jnp.dot(m_refs[d][me ^ j], p_all[me ^ d], preferred_element_type=jnp.float32)
            hid_ref[j] = total + b_refs[j][:, 3 * cols :].astype(jnp.float32)
        for j in range(count):
            at = pl.multiple_of(margin + (1 + rows * (me ^ j)) * STRIDE, 8)
            for r in range(rows):
                wide_ref[pl.ds(at + r * STRIDE, COLS), :] = hid_ref[j, r * COLS : (r + 1) * COLS, :]
        span = (grid_rows + 2) * STRIDE
        for dc in range(TAPS):
            near_ref[dc] = wide_ref[margin + dc - 1 : margin + dc - 1 + span, :].astype(jnp.bfloat16)
        for j in range(count):
            acc = 0.0
            for dr in range(TAPS):
                for dc in range(TAPS):
                    at = (rows * j + dr) * STRIDE
                    acc = acc + jnp.dot(
                        near_ref[dc, at : at + rows * STRIDE, :], t_all[dr * TAPS + dc], preferred_element_type=jnp.float32
                    )
            role = me ^ j

            @pl.when(role % 2 == 0)
            def _():
                even_ref[role // 2] = acc

            @pl.when(role % 2 == 1)
            def _():
                odd_ref[role // 2] = acc.astype(odd_ref.dtype)

    span = (grid_rows + 2) * STRIDE
    return pl.pallas_call(
        kernel,
        out_shape=(
            jax.ShapeDtypeStruct((count // 2, rows * STRIDE, feat_out), jnp.float32),
            jax.ShapeDtypeStruct((count // 2, rows * STRIDE, feat_out), jnp.bfloat16),
        ),
        in_specs=[pl.BlockSpec(memory_space=pltpu.SMEM)]
        + [pl.BlockSpec(memory_space=pltpu.VMEM)] * (2 * count + parts + len(tap_parts)),
        scratch_shapes=[
            pltpu.VMEM((count, cols, quarter), jnp.bfloat16),
            pltpu.VMEM((TAPS * TAPS, quarter, feat_out), jnp.bfloat16),
            pltpu.VMEM((count, tokens, quarter), jnp.float32),
            pltpu.VMEM((span + 2 * margin, quarter), jnp.float32),
            pltpu.VMEM((TAPS, span, quarter), jnp.bfloat16),
        ],
        name="project_and_convolve",
    )(scalars, *mixed, *blocks, *proj_parts, *tap_parts)


def body(queries, key_states, value_states, residual, proj_weight, conv_weight):
    tokens, width = queries.shape[1:]
    quarter = proj_weight.shape[1]
    feat_out = conv_weight.shape[3]
    count = lax.axis_size("blk")
    assert lax.axis_size("batch") == count and lax.axis_size("groups") == 2
    me = lax.axis_index("blk")
    depth = lax.axis_index("batch")
    side = lax.axis_index("groups")
    high = count.bit_length() - 2

    def turned(k):
        return (k >> 1) | ((k & 1) << high)

    scalars = jnp.stack([me, side] + [depth ^ turned(me ^ d) for d in range(count)]).astype(jnp.int32)

    def across(x, offset):
        return lax.ppermute(x, "blk", [(i, i ^ offset) for i in range(count)])

    def from_row(x):
        pairs = [((z ^ turned(k)) * count + k, z * count + k) for z in range(count) for k in range(count)]
        return lax.ppermute(x, ("batch", "blk"), pairs)

    def from_group(x):
        return lax.ppermute(x, "groups", [(0, 1), (1, 0)])

    taps = conv_weight.reshape(TAPS * TAPS, quarter, feat_out)
    if quarter // 2 % 16 == 0:
        proj_half = lax.dynamic_slice_in_dim(proj_weight, side * (width // 2), width // 2, axis=0)
        taps_half = lax.dynamic_slice_in_dim(taps, side * (quarter // 2), quarter // 2, axis=1)
        to_send = [proj_half] + [taps_half[t0:t1] for t0, t1 in CHUNKS]
    else:
        to_send = [proj_weight] + [taps[t0:t1] for t0, t1 in CHUNKS]

    sends = pack(scalars, queries[0], key_states[0], value_states[0], residual[0], count)
    blocks = [sends[0]] + [across(sends[d], d) for d in range(1, count)]
    fetched = [from_row(x) for x in to_send]
    if quarter // 2 % 16 == 0:
        parts = [(x, from_group(x)) for x in fetched]
    else:
        parts = [(x,) for x in fetched]

    cols = width // count
    mixed = [attention(scalars, blocks, cols)]
    offset = count // 2
    offsets = [0]
    while offset:
        mixed = mixed + [across(x, offset) for x in mixed]
        offsets = offsets + [o ^ offset for o in offsets]
        offset //= 2
    mixed = [mixed[offsets.index(d)] for d in range(count)]

    even, odd = project_and_convolve(
        scalars, mixed, blocks, parts[0], [x for pair in parts[1:] for x in pair], feat_out
    )
    summed = even + across(odd, 1).astype(jnp.float32)
    offset = 2
    while offset < count:
        summed = summed[0::2] + across(summed[1::2].astype(jnp.bfloat16), offset).astype(jnp.float32)
        offset *= 2
    rows = tokens // COLS
    return summed[0].reshape(rows, STRIDE, feat_out)[:, :COLS].reshape(1, tokens, feat_out).astype(jnp.bfloat16)


def solution(mesh):
    return jax.shard_map(
        body,
        mesh=mesh,
        in_specs=(
            P(("groups", "batch"), "blk", None),
            P(("groups", "batch"), "blk", None),
            P(("groups", "batch"), "blk", None),
            P(("groups", "batch"), "blk", None),
            P(None, "batch"),
            P(None, None, "batch", None),
        ),
        out_specs=P(("groups", "batch"), "blk", None),
        check_vma=False,
    )
```
